32 devices in a mesh: gy: 4 (over z), gx: 8 (over y, x, core).
Axes of the slice: x: 2, y: 2, z: 4, core: 2. Of those that a mesh axis runs over, the one named last changes fastest.
Arguments:
- coefficients: float32 [9, 128, 256], P(None, 'gy', 'gx'), may hold values from -2.1 to 2.1
- vectors: float32 [128, 256, 2048], P('gy', 'gx'), may hold values from -6 to 6
Outputs:
- normal: float32 [25, 128, 256], P(None, 'gy', 'gx')
- image: float32 [128, 256, 2048], P('gy', 'gx')
The draws below stay inside these ranges and needn't reach their ends.
All inputs are finite; a program needn't handle non-finite values.
Results may differ from the reference program's by a relative error of at most 0.00002.
Values sent between devices are 32-bit elements; how exact they have to be, the bound alone decides.
A program may use at most 192 MiB of HBM per device.

```python
import math
import jax
import jax.numpy as jnp
from jax import lax

NV = 2048
NX = 128
NY = 256


def block_levels(rng, shape, shards, least, largest):
    def one(axis_at, parts):
        heights = jax.random.uniform(jax.random.fold_in(jax.random.fold_in(rng, 6), axis_at), (parts,), jnp.float32, least / len(shards), largest / len(shards))
        return jnp.repeat(jnp.exp(heights), shape[axis_at] // parts).reshape((-1,) + (1,) * (len(shape) - axis_at - 1))

    loudness = one(*shards[0])
    for cut in shards[1:]:
        loudness = loudness * one(*cut)
    return loudness


def centred(stream_key, shape, spread, limit, cuts=(), held_as=jnp.bfloat16):
    gain = block_levels(stream_key, shape, cuts, -0.22, 0.18) if cuts else 1.0
    drawn = jax.random.normal(stream_key, shape, jnp.float32) * spread * gain
    return jnp.minimum(jnp.maximum(drawn, -limit), limit).astype(held_as)


def setup_inputs(seed: int = 0) -> dict:
    keys = jax.random.split(jax.random.key(seed), 3)
    coefficients = centred(keys[0], (9, NX, NY), 0.35, 2.1, ((1, 4), (2, 8)), jnp.float32)
    vectors = centred(keys[1], (NX, NY, NV), 1.0, 6.0, ((0, 4), (1, 8)), jnp.float32)
    return dict(coefficients=coefficients, vectors=vectors)


def reference(coefficients, vectors):
    row_pos = jnp.arange(NX, dtype=jnp.int32)[:, None]
    col_pos = jnp.arange(NY, dtype=jnp.int32)[None, :]
    pieces = []
    for k in range(9):
        a = k // 3 - 1
        b = k % 3 - 1
        inside = (row_pos + a >= 0) & (row_pos + a < NX) & (col_pos + b >= 0) & (col_pos + b < NY)
        pieces.append(jnp.where(inside, coefficients[k], jnp.zeros_like(coefficients[k])))
    masked = jnp.stack(pieces)
    padded = jnp.pad(masked, ((0, 0), (1, 1), (1, 1)))
    terms = [jnp.zeros((NX, NY), coefficients.dtype) for slot in range(25)]
    for k in range(9):
        a = k // 3 - 1
        b = k % 3 - 1
        for m in range(9):
            e = (m // 3) - (k // 3)
            f = (m % 3) - (k % 3)
            slot_index = (e + 2) * 5 + (f + 2)
            first = padded[k, 1 - a:1 - a + NX, 1 - b:1 - b + NY]
            second = padded[m, 1 - a:1 - a + NX, 1 - b:1 - b + NY]
            terms[slot_index] = terms[slot_index] + first * second
    normal = jnp.stack(terms)
    block = math.gcd(NV, 128)

    def one_block(step, image):
        part = lax.dynamic_slice_in_dim(vectors, step * block, block, 2)
        wide = jnp.pad(part, ((2, 2), (2, 2), (0, 0)))
        total = jnp.zeros((NX, NY, block), vectors.dtype)
        for e in range(-2, 3):
            for f in range(-2, 3):
                slot_index = (e + 2) * 5 + (f + 2)
                total = total + normal[slot_index][:, :, None] * wide[2 + e:2 + e + NX, 2 + f:2 + f + NY, :]
        return lax.dynamic_update_slice_in_dim(image, total, step * block, 2)

    image = lax.fori_loop(0, NV // block, one_block, jnp.zeros_like(vectors))
    return normal, image
```

```python
import functools
import jax
import jax.numpy as jnp
from jax import lax
from jax.experimental import pallas as pl
from jax.experimental.pallas import tpu as pltpu
from jax.sharding import PartitionSpec as P


GROUP = 4
CHUNKS = 2
LANES = 256


def moved(block, dy, dx):
    rows = lax.axis_size("gy")
    cols = lax.axis_size("gx")
    route = []
    for y in range(rows):
        for x in range(cols):
            if 0 <= y + dy < rows and 0 <= x + dx < cols:
                route.append((y * cols + x, (y + dy) * cols + x + dx))
    return lax.ppermute(block, ("gy", "gx"), route)


def edge(array, dim, side, width):
    size = array.shape[dim]
    if side > 0:
        return lax.slice_in_dim(array, size - width, size, axis=dim)
    return lax.slice_in_dim(array, 0, width, axis=dim)


def ring(array, dim, width):
    found = {}
    for dy in (1, -1):
        found[dy, 0] = moved(edge(array, dim, dy, width), dy, 0)
    for dx in (1, -1):
        found[0, dx] = moved(edge(array, dim + 1, dx, width), 0, dx)
    for dy in (1, -1):
        for dx in (1, -1):
            corner = edge(edge(array, dim, dy, width), dim + 1, dx, width)
            found[dy, dx] = moved(corner, dy, dx)
    return found


def masked_weights(coefficients):
    rows_dev = coefficients.shape[1]
    cols_dev = coefficients.shape[2]
    total_rows = rows_dev * lax.axis_size("gy")
    total_cols = cols_dev * lax.axis_size("gx")
    row_pos = lax.axis_index("gy") * rows_dev + jnp.arange(rows_dev, dtype=jnp.int32)[:, None]
    col_pos = lax.axis_index("gx") * cols_dev + jnp.arange(cols_dev, dtype=jnp.int32)[None, :]
    pieces = []
    for k in range(9):
        a = k // 3 - 1
        b = k % 3 - 1
        inside = (
            (row_pos + a >= 0)
            & (row_pos + a < total_rows)
            & (col_pos + b >= 0)
            & (col_pos + b < total_cols)
        )
        pieces.append(jnp.where(inside, coefficients[k], jnp.zeros_like(coefficients[k])))
    return jnp.stack(pieces)


def diagonals(ext, rows, cols, turned):
    terms = [None] * 25
    for k in range(9):
        a = k // 3 - 1
        b = k % 3 - 1
        if turned:
            at = (slice(1 - b, 1 - b + cols), slice(1 - a, 1 - a + rows))
        else:
            at = (slice(1 - a, 1 - a + rows), slice(1 - b, 1 - b + cols))
        first = ext[(k,) + at]
        for m in range(9):
            e = m // 3 - k // 3
            f = m % 3 - k % 3
            slot = (e + 2) * 5 + (f + 2)
            product = first * ext[(m,) + at]
            terms[slot] = product if terms[slot] is None else terms[slot] + product
    return terms


def band_kernel(rows, cols, ext_ref, turned_ref, normal_ref, high_ref, low_ref, halo_ref):
    for slot, term in enumerate(diagonals(ext_ref, rows, cols, False)):
        normal_ref[slot] = term
    columns = diagonals(turned_ref, rows, cols, True)
    deep = (GROUP + 4) * cols
    wide = (GROUP + 4) * 16
    shape = (cols, deep + wide)
    lane = lax.broadcasted_iota(jnp.int32, shape, 1)
    own = lax.broadcasted_iota(jnp.int32, shape, 0)
    beside = lane - deep
    is_main = lane < deep
    part = beside % 16
    near = part % 4
    source_row = jnp.where(is_main, lane // cols, beside // 16)
    source_col = jnp.where(is_main, lane % cols, jnp.where(near < 2, near - 2, near - 2 + cols))
    f = source_col - own
    usable = (f >= -2) & (f <= 2) & (is_main | (part < 12))
    takes_high = part < 8
    for rr in range(GROUP):
        e = source_row - 2 - rr
        code = jnp.where(usable & (e >= -2) & (e <= 2), (e + 2) * 5 + f + 2, -1)
        for r in range(rr, rows, GROUP):
            total = jnp.zeros(shape, jnp.float32)
            for slot in range(25):
                column = columns[slot][:, r : r + 1]
                total = jnp.where(code == slot, column, total)
            high = total.astype(jnp.bfloat16)
            rest = total - high.astype(jnp.float32)
            low = rest.astype(jnp.bfloat16)
            at = pl.ds(r * cols, cols)
            high_ref[at, :] = high[:, :deep]
            low_ref[at, :] = low[:, :deep]
            mixed = jnp.where(takes_high, high.astype(jnp.float32), rest)
            halo_ref[at, :] = mixed[:, deep:].astype(jnp.bfloat16)


def band_matrices(ext, rows, cols):
    deep = (GROUP + 4) * cols
    wide = (GROUP + 4) * 16
    cells = rows * cols
    turned = jnp.swapaxes(ext, 1, 2)
    return pl.pallas_call(
        functools.partial(band_kernel, rows, cols),
        out_shape=(
            jax.ShapeDtypeStruct((25, rows, cols), jnp.float32),
            jax.ShapeDtypeStruct((cells, deep), jnp.bfloat16),
            jax.ShapeDtypeStruct((cells, deep), jnp.bfloat16),
            jax.ShapeDtypeStruct((cells, wide), jnp.bfloat16),
        ),
        in_specs=[pl.BlockSpec(memory_space=pltpu.VMEM)] * 2,
        out_specs=(pl.BlockSpec(memory_space=pltpu.VMEM),) * 4,
        cost_estimate=pl.CostEstimate(flops=10_000_000, bytes_accessed=2_000_000, transcendentals=0),
    )(ext, turned)


def image_kernel(aliased, *refs):
    (x_ref, up_ref, down_ref, left_ref, right_ref, ul_ref, ur_ref, dl_ref, dr_ref) = refs[:9]
    high_ref, low_ref, mixed_ref = refs[9:12]
    rest = refs[12 + aliased :]
    out_ref, xh, xl, side, xs = rest
    rows, cols, lanes = x_ref.shape

    @pl.when(pl.program_id(0) == 0)
    def _():
        side[...] = jnp.zeros_like(side)

    def place(row, block):
        high = block.astype(jnp.bfloat16)
        low = (block - high.astype(jnp.float32)).astype(jnp.bfloat16)
        xh[pl.ds(row, block.shape[0])] = high
        xl[pl.ds(row, block.shape[0])] = low

    place(0, up_ref[...])
    place(rows + 2, down_ref[...])
    for r in range(0, rows, 4):
        place(r + 2, x_ref[r : r + 4])
    for copy in range(3):
        for at, top, mid, bottom in ((0, ul_ref, left_ref, dl_ref), (2, ur_ref, right_ref, dr_ref)):
            spot = pl.ds(4 * copy + at, 2)
            side[0:2, spot] = top[...]
            side[2 : rows + 2, spot] = mid[...]
            side[rows + 2 : rows + 4, spot] = bottom[...]
    for r in range(0, rows + 4, 4):
        raw = side[r : r + 4]
        slot = lax.broadcasted_iota(jnp.int32, raw.shape, 1)
        high = raw.astype(jnp.bfloat16).astype(jnp.float32)
        value = jnp.where((slot >= 4) & (slot < 8), raw - high, high)
        xs[r : r + 4] = value.astype(jnp.bfloat16)
    dot = functools.partial(jnp.dot, preferred_element_type=jnp.float32)
    for g in range(rows // GROUP):
        at = pl.ds(g * GROUP * cols, GROUP * cols)
        span = pl.ds(g * GROUP, GROUP + 4)
        h = xh[span].reshape((GROUP + 4) * cols, lanes)
        l = xl[span].reshape((GROUP + 4) * cols, lanes)
        s = xs[span].reshape((GROUP + 4) * 16, lanes)
        total = dot(high_ref[at, :], h) + dot(low_ref[at, :], h)
        total = total + dot(high_ref[at, :], l) + dot(mixed_ref[at, :], s)
        out_ref[pl.ds(g * GROUP, GROUP)] = total.reshape(GROUP, cols, lanes)


def image_chunk(vectors, found, bands, image, chunk, chunk_lanes):
    rows, cols, _ = vectors.shape
    steps = chunk_lanes // LANES
    first = chunk * steps
    halos = [
        found[1, 0], found[-1, 0], found[0, 1], found[0, -1],
        found[1, 1], found[1, -1], found[-1, 1], found[-1, -1],
    ]
    in_specs = [pl.BlockSpec((rows, cols, LANES), lambda j: (0, 0, j + first))]
    in_specs += [pl.BlockSpec(h.shape[:2] + (LANES,), lambda j: (0, 0, j)) for h in halos]
    in_specs += [pl.BlockSpec(b.shape, lambda j: (0, 0)) for b in bands]
    operands = [vectors] + halos + list(bands)
    aliases = {}
    if image is not None:
        aliases = {len(operands): 0}
        operands.append(image)
        in_specs.append(pl.BlockSpec(memory_space=pl.ANY))
    cells = rows * cols * chunk_lanes
    return pl.pallas_call(
        functools.partial(image_kernel, len(aliases)),
        grid=(steps,),
        out_shape=jax.ShapeDtypeStruct(vectors.shape, vectors.dtype),
        in_specs=in_specs,
        out_specs=pl.BlockSpec((rows, cols, LANES), lambda j: (0, 0, j + first)),
        scratch_shapes=[
            pltpu.VMEM((rows + 4, cols, LANES), jnp.bfloat16),
            pltpu.VMEM((rows + 4, cols, LANES), jnp.bfloat16),
            pltpu.VMEM((rows + 4, 16, LANES), jnp.float32),
            pltpu.VMEM((rows + 4, 16, LANES), jnp.bfloat16),
        ],
        input_output_aliases=aliases,
        cost_estimate=pl.CostEstimate(flops=cells * 2048, bytes_accessed=cells * 8, transcendentals=0),
        compiler_params=pltpu.CompilerParams(dimension_semantics=("arbitrary",)),
    )(*operands)


def per_device(coefficients, vectors):
    rows, cols, count = vectors.shape
    masked = masked_weights(coefficients)
    near = ring(masked, 1, 1)
    chunk_lanes = count // CHUNKS
    found = [
        ring(lax.slice_in_dim(vectors, c * chunk_lanes, (c + 1) * chunk_lanes, axis=2), 0, 2)
        for c in range(CHUNKS)
    ]
    ext = jnp.concatenate(
        [
            jnp.concatenate([near[dy, 1], near[dy, 0] if dy else masked, near[dy, -1]], axis=2)
            for dy in (1, 0, -1)
        ],
        axis=1,
    )
    normal, *bands = band_matrices(ext, rows, cols)
    image = None
    for c in range(CHUNKS):
        image = image_chunk(vectors, found[c], bands, image, c, chunk_lanes)
    return (normal, image)


def solution(mesh):
    in_specs = (P(None, "gy", "gx"), P("gy", "gx", None))
    out_specs = (P(None, "gy", "gx"), P("gy", "gx", None))
    return jax.shard_map(
        per_device, mesh=mesh, in_specs=in_specs, out_specs=out_specs, check_vma=False
    )
```

```python
import functools
import jax
import jax.numpy as jnp
from jax import lax
from jax.experimental import pallas as pl
from jax.experimental.pallas import tpu as pltpu
from jax.sharding import PartitionSpec as P

MESH = pl.DeviceIdType.MESH
GROUP = 4
LANES = 256


DIRECTIONS = ((1, 0), (-1, 0), (0, 1), (0, -1), (1, 1), (1, -1), (-1, 1), (-1, -1))


def exchange_kernel(ny, nx, x_ref, first_ref, last_ref, strips_ref, up, down, left, right, near, zero, *sems):
    send_sem, recv_sem, strip_send, strip_recv, fill_sem = sems
    rows = x_ref.shape[0]
    gy = lax.axis_index("gy")
    gx = lax.axis_index("gx")

    def there(dy, dx):
        y = gy + dy
        x = gx + dx
        return (y >= 0) & (y < ny) & (x >= 0) & (x < nx)

    barrier = pltpu.get_barrier_semaphore()
    count = jnp.int32(0)
    for dy, dx in DIRECTIONS:
        count = count + there(dy, dx).astype(jnp.int32)

        @pl.when(there(dy, dx))
        def _():
            pl.semaphore_signal(barrier, inc=1, device_id={"gy": gy + dy, "gx": gx + dx}, device_id_type=MESH)

    pl.semaphore_wait(barrier, count)

    mine = {1: pl.ds(rows - 2, 2), -1: pl.ds(0, 2)}
    land = {1: pl.ds(0, 2), 0: pl.ds(2, rows), -1: pl.ds(rows + 2, 2)}
    jobs = []
    for d, (dy, dx) in enumerate(DIRECTIONS):
        to = {"gy": gy + dy, "gx": gx + dx}
        if dx == 0:
            source = x_ref.at[mine[dy]]
            target = up if dy > 0 else down
        else:
            column = last_ref if dx > 0 else first_ref
            source = column.at[mine[dy]] if dy else column
            target = (left if dx > 0 else right).at[land[dy]]
        strip = (dy + 1) // 2 if dy else 2 + (dx + 1) // 2
        small = pltpu.make_async_remote_copy(
            strips_ref.at[strip], near.at[d], strip_send.at[d], strip_recv.at[d],
            device_id=to, device_id_type=MESH,
        )
        large = pltpu.make_async_remote_copy(
            source, target, send_sem.at[d], recv_sem.at[d], device_id=to, device_id_type=MESH
        )
        fill = None
        if dx:
            zeros = zero.at[pl.ds(0, 2)] if dy else zero
            fill = pltpu.make_async_copy(zeros, target, fill_sem.at[d])
        jobs.append((dy, dx, small, large, fill))

    for dy, dx, small, large, fill in jobs:

        @pl.when(there(dy, dx))
        def _():
            small.start()
            large.start()

    zero[...] = jnp.zeros_like(zero)
    for dy, dx, small, large, fill in jobs:

        if fill is None:
            continue

        @pl.when(jnp.logical_not(there(-dy, -dx)))
        def _():
            fill.start()
            fill.wait()

    for dy, dx, small, large, fill in jobs:

        @pl.when(there(dy, dx))
        def _():
            small.wait_send()
            large.wait_send()

        @pl.when(there(-dy, -dx))
        def _():
            small.wait_recv()
            large.wait_recv()


def exchange(vectors, masked):
    rows, cols, count = vectors.shape
    ny = lax.axis_size("gy")
    nx = lax.axis_size("gx")
    strips = jnp.stack([masked[:, 0, :], masked[:, -1, :], masked[:, :, 0], masked[:, :, -1]])
    strips = jnp.pad(strips, ((0, 0), (0, 7), (0, 128 - strips.shape[2])))
    any_space = pl.BlockSpec(memory_space=pl.ANY)
    real = jnp.float32
    sems = [pltpu.SemaphoreType.DMA((8,))] * 5
    up, down, left, right, near = pl.pallas_call(
        functools.partial(exchange_kernel, ny, nx),
        out_shape=(
            jax.ShapeDtypeStruct((2, cols, count), real),
            jax.ShapeDtypeStruct((2, cols, count), real),
            jax.ShapeDtypeStruct((rows + 4, 2, count), real),
            jax.ShapeDtypeStruct((rows + 4, 2, count), real),
            jax.ShapeDtypeStruct((8,) + strips.shape[1:], real),
        ),
        in_specs=[any_space] * 4,
        out_specs=(any_space,) * 5,
        scratch_shapes=[pltpu.VMEM((rows, 2, count), real)] + sems,
        compiler_params=pltpu.CompilerParams(collective_id=0, has_side_effects=True),
    )(vectors, vectors[:, :2], vectors[:, -2:], strips)
    gy = lax.axis_index("gy")
    gx = lax.axis_index("gx")
    found = {}
    for d, (dy, dx) in enumerate(DIRECTIONS):
        y = gy - dy
        x = gx - dx
        there = (y >= 0) & (y < ny) & (x >= 0) & (x < nx)
        strip = jnp.where(there, near[d, :9], 0)
        if dy == 0:
            found[dy, dx] = strip[:, :rows, None]
        elif dx == 0:
            found[dy, dx] = strip[:, None, :cols]
        else:
            at = cols - 1 if dx > 0 else 0
            found[dy, dx] = strip[:, None, at : at + 1]
    return (up, down, left, right), found


def masked_weights(coefficients):
    rows_dev = coefficients.shape[1]
    cols_dev = coefficients.shape[2]
    total_rows = rows_dev * lax.axis_size("gy")
    total_cols = cols_dev * lax.axis_size("gx")
    row_pos = lax.axis_index("gy") * rows_dev + jnp.arange(rows_dev, dtype=jnp.int32)[:, None]
    col_pos = lax.axis_index("gx") * cols_dev + jnp.arange(cols_dev, dtype=jnp.int32)[None, :]
    pieces = []
    for k in range(9):
        a = k // 3 - 1
        b = k % 3 - 1
        inside = (
            (row_pos + a >= 0)
            & (row_pos + a < total_rows)
            & (col_pos + b >= 0)
            & (col_pos + b < total_cols)
        )
        pieces.append(jnp.where(inside, coefficients[k], jnp.zeros_like(coefficients[k])))
    return jnp.stack(pieces)


def diagonals(ext, rows, cols, turned):
    terms = [None] * 25
    for k in range(9):
        a = k // 3 - 1
        b = k % 3 - 1
        if turned:
            at = (slice(1 - b, 1 - b + cols), slice(1 - a, 1 - a + rows))
        else:
            at = (slice(1 - a, 1 - a + rows), slice(1 - b, 1 - b + cols))
        first = ext[(k,) + at]
        for m in range(9):
            e = m // 3 - k // 3
            f = m % 3 - k % 3
            slot = (e + 2) * 5 + (f + 2)
            product = first * ext[(m,) + at]
            terms[slot] = product if terms[slot] is None else terms[slot] + product
    return terms


def band_kernel(rows, cols, ext_ref, turned_ref, normal_ref, high_ref, low_ref, halo_ref):
    for slot, term in enumerate(diagonals(ext_ref, rows, cols, False)):
        normal_ref[slot] = term
    columns = diagonals(turned_ref, rows, cols, True)
    deep = (GROUP + 4) * cols
    wide = (GROUP + 4) * 16
    shape = (cols, deep + wide)
    lane = lax.broadcasted_iota(jnp.int32, shape, 1)
    own = lax.broadcasted_iota(jnp.int32, shape, 0)
    beside = lane - deep
    is_main = lane < deep
    part = beside % 16
    near = part % 4
    source_row = jnp.where(is_main, lane // cols, beside // 16)
    source_col = jnp.where(is_main, lane % cols, jnp.where(near < 2, near - 2, near - 2 + cols))
    f = source_col - own
    usable = (f >= -2) & (f <= 2) & (is_main | (part < 12))
    takes_high = part < 8
    for rr in range(GROUP):
        e = source_row - 2 - rr
        code = jnp.where(usable & (e >= -2) & (e <= 2), (e + 2) * 5 + f + 2, -1)
        for r in range(rr, rows, GROUP):
            total = jnp.zeros(shape, jnp.float32)
            for slot in range(25):
                column = columns[slot][:, r : r + 1]
                total = jnp.where(code == slot, column, total)
            high = total.astype(jnp.bfloat16)
            rest = total - high.astype(jnp.float32)
            low = rest.astype(jnp.bfloat16)
            at = pl.ds(r * cols, cols)
            high_ref[at, :] = high[:, :deep]
            low_ref[at, :] = low[:, :deep]
            mixed = jnp.where(takes_high, high.astype(jnp.float32), rest)
            halo_ref[at, :] = mixed[:, deep:].astype(jnp.bfloat16)


def band_matrices(ext, rows, cols):
    deep = (GROUP + 4) * cols
    wide = (GROUP + 4) * 16
    cells = rows * cols
    turned = jnp.swapaxes(ext, 1, 2)
    return pl.pallas_call(
        functools.partial(band_kernel, rows, cols),
        out_shape=(
            jax.ShapeDtypeStruct((25, rows, cols), jnp.float32),
            jax.ShapeDtypeStruct((cells, deep), jnp.bfloat16),
            jax.ShapeDtypeStruct((cells, deep), jnp.bfloat16),
            jax.ShapeDtypeStruct((cells, wide), jnp.bfloat16),
        ),
        in_specs=[pl.BlockSpec(memory_space=pltpu.VMEM)] * 2,
        out_specs=(pl.BlockSpec(memory_space=pltpu.VMEM),) * 4,
        cost_estimate=pl.CostEstimate(flops=10_000_000, bytes_accessed=2_000_000, transcendentals=0),
    )(ext, turned)


def image_kernel(*refs):
    x_ref, up_ref, down_ref, left_ref, right_ref, high_ref, low_ref, mixed_ref = refs[:8]
    out_ref, xh, xl, side, xs = refs[8:]
    rows, cols, lanes = x_ref.shape

    @pl.when(pl.program_id(0) == 0)
    def _():
        side[...] = jnp.zeros_like(side)

    def place(row, block):
        high = block.astype(jnp.bfloat16)
        low = (block - high.astype(jnp.float32)).astype(jnp.bfloat16)
        xh[pl.ds(row, block.shape[0])] = high
        xl[pl.ds(row, block.shape[0])] = low

    gy = lax.axis_index("gy")
    has_up = gy > 0
    has_down = gy < lax.axis_size("gy") - 1
    place(0, jnp.where(has_up, up_ref[...], 0))
    place(rows + 2, jnp.where(has_down, down_ref[...], 0))
    for r in range(0, rows, 4):
        place(r + 2, x_ref[r : r + 4])
    for copy in range(3):
        side[:, pl.ds(4 * copy, 2)] = left_ref[...]
        side[:, pl.ds(4 * copy + 2, 2)] = right_ref[...]
    for r in range(0, rows + 4, 4):
        raw = side[r : r + 4]
        slot = lax.broadcasted_iota(jnp.int32, raw.shape, 1)
        high = raw.astype(jnp.bfloat16).astype(jnp.float32)
        value = jnp.where((slot >= 4) & (slot < 8), raw - high, high)
        xs[r : r + 4] = value.astype(jnp.bfloat16)
    dot = functools.partial(jnp.dot, preferred_element_type=jnp.float32)
    for g in range(rows // GROUP):
        at = pl.ds(g * GROUP * cols, GROUP * cols)
        span = pl.ds(g * GROUP, GROUP + 4)
        h = xh[span].reshape((GROUP + 4) * cols, lanes)
        l = xl[span].reshape((GROUP + 4) * cols, lanes)
        s = xs[span].reshape((GROUP + 4) * 16, lanes)
        total = dot(high_ref[at, :], h) + dot(low_ref[at, :], h)
        total = total + dot(high_ref[at, :], l) + dot(mixed_ref[at, :], s)
        out_ref[pl.ds(g * GROUP, GROUP)] = total.reshape(GROUP, cols, lanes)


def image_of(vectors, halos, bands):
    rows, cols, count = vectors.shape
    blocks = [vectors, *halos]
    cells = rows * cols * count
    return pl.pallas_call(
        image_kernel,
        grid=(count // LANES,),
        out_shape=jax.ShapeDtypeStruct(vectors.shape, vectors.dtype),
        in_specs=[pl.BlockSpec(h.shape[:2] + (LANES,), lambda j: (0, 0, j)) for h in blocks]
        + [pl.BlockSpec(b.shape, lambda j: (0, 0)) for b in bands],
        out_specs=pl.BlockSpec((rows, cols, LANES), lambda j: (0, 0, j)),
        scratch_shapes=[
            pltpu.VMEM((rows + 4, cols, LANES), jnp.bfloat16),
            pltpu.VMEM((rows + 4, cols, LANES), jnp.bfloat16),
            pltpu.VMEM((rows + 4, 16, LANES), jnp.float32),
            pltpu.VMEM((rows + 4, 16, LANES), jnp.bfloat16),
        ],
        cost_estimate=pl.CostEstimate(flops=cells * 2048, bytes_accessed=cells * 8, transcendentals=0),
        compiler_params=pltpu.CompilerParams(dimension_semantics=("arbitrary",)),
    )(*blocks, *bands)


def per_device(coefficients, vectors):
    rows, cols, _ = vectors.shape
    masked = masked_weights(coefficients)
    halos, near = exchange(vectors, masked)
    ext = jnp.concatenate(
        [
            jnp.concatenate([near[dy, 1], near[dy, 0] if dy else masked, near[dy, -1]], axis=2)
            for dy in (1, 0, -1)
        ],
        axis=1,
    )
    normal, *bands = band_matrices(ext, rows, cols)
    image = image_of(vectors, halos, bands)
    return (normal, image)


def solution(mesh):
    in_specs = (P(None, "gy", "gx"), P("gy", "gx", None))
    out_specs = (P(None, "gy", "gx"), P("gy", "gx", None))
    return jax.shard_map(
        per_device, mesh=mesh, in_specs=in_specs, out_specs=out_specs, check_vma=False
    )
```

```python
import functools
import jax
import jax.numpy as jnp
from jax import lax
from jax.experimental import pallas as pl
from jax.experimental.pallas import tpu as pltpu
from jax.sharding import PartitionSpec as P

MESH = pl.DeviceIdType.MESH
GROUP = 4
LANES = 256


DIRECTIONS = ((1, 0), (-1, 0), (0, 1), (0, -1), (1, 1), (1, -1), (-1, 1), (-1, -1))


def exchange_kernel(ny, nx, x_ref, strips_ref, up, down, left, right, near, zero, *sems):
    send_sem, recv_sem, strip_send, strip_recv, fill_sem = sems
    rows, cols, _ = x_ref.shape
    gy = lax.axis_index("gy")
    gx = lax.axis_index("gx")

    def there(dy, dx):
        y = gy + dy
        x = gx + dx
        return (y >= 0) & (y < ny) & (x >= 0) & (x < nx)

    barrier = pltpu.get_barrier_semaphore()
    count = jnp.int32(0)
    for dy, dx in DIRECTIONS:
        count = count + there(dy, dx).astype(jnp.int32)

        @pl.when(there(dy, dx))
        def _():
            pl.semaphore_signal(barrier, inc=1, device_id={"gy": gy + dy, "gx": gx + dx}, device_id_type=MESH)

    pl.semaphore_wait(barrier, count)

    mine = {1: pl.ds(rows - 2, 2), -1: pl.ds(0, 2)}
    land = {1: pl.ds(0, 2), 0: pl.ds(2, rows), -1: pl.ds(rows + 2, 2)}
    jobs = []
    for d, (dy, dx) in enumerate(DIRECTIONS):
        to = {"gy": gy + dy, "gx": gx + dx}
        if dx == 0:
            source = x_ref.at[mine[dy]]
            target = up if dy > 0 else down
        else:
            lines = mine[dy] if dy else pl.ds(0, rows)
            source = x_ref.at[lines, pl.ds(cols - 2 if dx > 0 else 0, 2)]
            target = (left if dx > 0 else right).at[land[dy]]
        strip = (dy + 1) // 2 if dy else 2 + (dx + 1) // 2
        small = pltpu.make_async_remote_copy(
            strips_ref.at[strip], near.at[d], strip_send.at[d], strip_recv.at[d],
            device_id=to, device_id_type=MESH,
        )
        large = pltpu.make_async_remote_copy(
            source, target, send_sem.at[d], recv_sem.at[d], device_id=to, device_id_type=MESH
        )
        fill = None
        if dx:
            zeros = zero.at[pl.ds(0, 2)] if dy else zero
            fill = pltpu.make_async_copy(zeros, target, fill_sem.at[d])
        jobs.append((dy, dx, small, large, fill))

    for dy, dx, small, large, fill in jobs:

        @pl.when(there(dy, dx))
        def _():
            small.start()
            large.start()

    zero[...] = jnp.zeros_like(zero)
    for dy, dx, small, large, fill in jobs:

        if fill is None:
            continue

        @pl.when(jnp.logical_not(there(-dy, -dx)))
        def _():
            fill.start()
            fill.wait()

    for dy, dx, small, large, fill in jobs:

        @pl.when(there(dy, dx))
        def _():
            small.wait_send()
            large.wait_send()

        @pl.when(there(-dy, -dx))
        def _():
            small.wait_recv()
            large.wait_recv()


def exchange(vectors, masked):
    rows, cols, count = vectors.shape
    ny = lax.axis_size("gy")
    nx = lax.axis_size("gx")
    strips = jnp.stack([masked[:, 0, :], masked[:, -1, :], masked[:, :, 0], masked[:, :, -1]])
    strips = jnp.pad(strips, ((0, 0), (0, 7), (0, 128 - strips.shape[2])))
    any_space = pl.BlockSpec(memory_space=pl.ANY)
    real = jnp.float32
    sems = [pltpu.SemaphoreType.DMA((8,))] * 5
    up, down, left, right, near = pl.pallas_call(
        functools.partial(exchange_kernel, ny, nx),
        out_shape=(
            jax.ShapeDtypeStruct((2, cols, count), real),
            jax.ShapeDtypeStruct((2, cols, count), real),
            jax.ShapeDtypeStruct((rows + 4, 2, count), real),
            jax.ShapeDtypeStruct((rows + 4, 2, count), real),
            jax.ShapeDtypeStruct((8,) + strips.shape[1:], real),
        ),
        in_specs=[any_space] * 2,
        out_specs=(any_space,) * 5,
        scratch_shapes=[pltpu.VMEM((rows, 2, count), real)] + sems,
        compiler_params=pltpu.CompilerParams(collective_id=0, has_side_effects=True),
    )(vectors, strips)
    gy = lax.axis_index("gy")
    gx = lax.axis_index("gx")
    found = {}
    for d, (dy, dx) in enumerate(DIRECTIONS):
        y = gy - dy
        x = gx - dx
        there = (y >= 0) & (y < ny) & (x >= 0) & (x < nx)
        strip = jnp.where(there, near[d, :9], 0)
        if dy == 0:
            found[dy, dx] = strip[:, :rows, None]
        elif dx == 0:
            found[dy, dx] = strip[:, None, :cols]
        else:
            at = cols - 1 if dx > 0 else 0
            found[dy, dx] = strip[:, None, at : at + 1]
    return (up, down, left, right), found


def masked_weights(coefficients):
    rows_dev = coefficients.shape[1]
    cols_dev = coefficients.shape[2]
    total_rows = rows_dev * lax.axis_size("gy")
    total_cols = cols_dev * lax.axis_size("gx")
    row_pos = lax.axis_index("gy") * rows_dev + jnp.arange(rows_dev, dtype=jnp.int32)[:, None]
    col_pos = lax.axis_index("gx") * cols_dev + jnp.arange(cols_dev, dtype=jnp.int32)[None, :]
    pieces = []
    for k in range(9):
        a = k // 3 - 1
        b = k % 3 - 1
        inside = (
            (row_pos + a >= 0)
            & (row_pos + a < total_rows)
            & (col_pos + b >= 0)
            & (col_pos + b < total_cols)
        )
        pieces.append(jnp.where(inside, coefficients[k], jnp.zeros_like(coefficients[k])))
    return jnp.stack(pieces)


def diagonals(ext, rows, cols, turned):
    terms = [None] * 25
    for k in range(9):
        a = k // 3 - 1
        b = k % 3 - 1
        if turned:
            at = (slice(1 - b, 1 - b + cols), slice(1 - a, 1 - a + rows))
        else:
            at = (slice(1 - a, 1 - a + rows), slice(1 - b, 1 - b + cols))
        first = ext[(k,) + at]
        for m in range(9):
            e = m // 3 - k // 3
            f = m % 3 - k % 3
            slot = (e + 2) * 5 + (f + 2)
            product = first * ext[(m,) + at]
            terms[slot] = product if terms[slot] is None else terms[slot] + product
    return terms


def band_kernel(rows, cols, ext_ref, turned_ref, normal_ref, high_ref, low_ref, halo_ref):
    for slot, term in enumerate(diagonals(ext_ref, rows, cols, False)):
        normal_ref[slot] = term
    columns = diagonals(turned_ref, rows, cols, True)
    deep = (GROUP + 4) * cols
    wide = (GROUP + 4) * 16
    shape = (cols, deep + wide)
    lane = lax.broadcasted_iota(jnp.int32, shape, 1)
    own = lax.broadcasted_iota(jnp.int32, shape, 0)
    beside = lane - deep
    is_main = lane < deep
    part = beside % 16
    near = part % 4
    source_row = jnp.where(is_main, lane // cols, beside // 16)
    source_col = jnp.where(is_main, lane % cols, jnp.where(near < 2, near - 2, near - 2 + cols))
    f = source_col - own
    usable = (f >= -2) & (f <= 2) & (is_main | (part < 12))
    takes_high = part < 8
    for rr in range(GROUP):
        e = source_row - 2 - rr
        code = jnp.where(usable & (e >= -2) & (e <= 2), (e + 2) * 5 + f + 2, -1)
        codes = [code[:, n : n + 128] for n in range(0, deep + wide, 128)]
        for r in range(rr, rows, GROUP):
            parts = [jnp.zeros((cols, 128), jnp.float32)] * len(codes)
            for slot in range(25):
                column = columns[slot][:, r : r + 1]
                line = slot // 5 + rr
                touched = {line * cols // 128, (line * cols + cols - 1) // 128}
                if slot % 5 != 2:
                    touched.add((deep + line * 16) // 128)
                for n in sorted(touched):
                    parts[n] = jnp.where(codes[n] == slot, column, parts[n])
            total = jnp.concatenate(parts, axis=1)
            high = total.astype(jnp.bfloat16)
            rest = total - high.astype(jnp.float32)
            low = rest.astype(jnp.bfloat16)
            at = pl.ds(r * cols, cols)
            high_ref[at, :] = high[:, :deep]
            low_ref[at, :] = low[:, :deep]
            mixed = jnp.where(takes_high, high.astype(jnp.float32), rest)
            halo_ref[at, :] = mixed[:, deep:].astype(jnp.bfloat16)


def band_matrices(ext, rows, cols):
    deep = (GROUP + 4) * cols
    wide = (GROUP + 4) * 16
    cells = rows * cols
    turned = jnp.swapaxes(ext, 1, 2)
    return pl.pallas_call(
        functools.partial(band_kernel, rows, cols),
        out_shape=(
            jax.ShapeDtypeStruct((25, rows, cols), jnp.float32),
            jax.ShapeDtypeStruct((cells, deep), jnp.bfloat16),
            jax.ShapeDtypeStruct((cells, deep), jnp.bfloat16),
            jax.ShapeDtypeStruct((cells, wide), jnp.bfloat16),
        ),
        in_specs=[pl.BlockSpec(memory_space=pltpu.VMEM)] * 2,
        out_specs=(pl.BlockSpec(memory_space=pltpu.VMEM),) * 4,
        cost_estimate=pl.CostEstimate(flops=10_000_000, bytes_accessed=2_000_000, transcendentals=0),
    )(ext, turned)


def image_kernel(*refs):
    x_ref, up_ref, down_ref, left_ref, right_ref, high_ref, low_ref, mixed_ref = refs[:8]
    out_ref, xh, xl, side, xs = refs[8:]
    rows, cols, lanes = x_ref.shape

    @pl.when(pl.program_id(0) == 0)
    def _():
        side[...] = jnp.zeros_like(side)

    def place(row, block):
        high = block.astype(jnp.bfloat16)
        low = (block - high.astype(jnp.float32)).astype(jnp.bfloat16)
        xh[pl.ds(row, block.shape[0])] = high
        xl[pl.ds(row, block.shape[0])] = low

    gy = lax.axis_index("gy")
    has_up = gy > 0
    has_down = gy < lax.axis_size("gy") - 1
    place(0, jnp.where(has_up, up_ref[...], 0))
    place(rows + 2, jnp.where(has_down, down_ref[...], 0))
    for r in range(0, rows, 4):
        place(r + 2, x_ref[r : r + 4])
    for copy in range(3):
        side[:, pl.ds(4 * copy, 2)] = left_ref[...]
        side[:, pl.ds(4 * copy + 2, 2)] = right_ref[...]
    for r in range(0, rows + 4, 4):
        raw = side[r : r + 4]
        slot = lax.broadcasted_iota(jnp.int32, raw.shape, 1)
        high = raw.astype(jnp.bfloat16).astype(jnp.float32)
        value = jnp.where((slot >= 4) & (slot < 8), raw - high, high)
        xs[r : r + 4] = value.astype(jnp.bfloat16)
    dot = functools.partial(jnp.dot, preferred_element_type=jnp.float32)
    for g in range(rows // GROUP):
        at = pl.ds(g * GROUP * cols, GROUP * cols)
        span = pl.ds(g * GROUP, GROUP + 4)
        h = xh[span].reshape((GROUP + 4) * cols, lanes)
        l = xl[span].reshape((GROUP + 4) * cols, lanes)
        s = xs[span].reshape((GROUP + 4) * 16, lanes)
        total = dot(high_ref[at, :], h) + dot(low_ref[at, :], h)
        total = total + dot(high_ref[at, :], l) + dot(mixed_ref[at, :], s)
        out_ref[pl.ds(g * GROUP, GROUP)] = total.reshape(GROUP, cols, lanes)


def image_of(vectors, halos, bands):
    rows, cols, count = vectors.shape
    blocks = [vectors, *halos]
    cells = rows * cols * count
    return pl.pallas_call(
        image_kernel,
        grid=(count // LANES,),
        out_shape=jax.ShapeDtypeStruct(vectors.shape, vectors.dtype),
        in_specs=[pl.BlockSpec(h.shape[:2] + (LANES,), lambda j: (0, 0, j)) for h in blocks]
        + [pl.BlockSpec(b.shape, lambda j: (0, 0)) for b in bands],
        out_specs=pl.BlockSpec((rows, cols, LANES), lambda j: (0, 0, j)),
        scratch_shapes=[
            pltpu.VMEM((rows + 4, cols, LANES), jnp.bfloat16),
            pltpu.VMEM((rows + 4, cols, LANES), jnp.bfloat16),
            pltpu.VMEM((rows + 4, 16, LANES), jnp.float32),
            pltpu.VMEM((rows + 4, 16, LANES), jnp.bfloat16),
        ],
        cost_estimate=pl.CostEstimate(flops=cells * 2048, bytes_accessed=cells * 8, transcendentals=0),
        compiler_params=pltpu.CompilerParams(dimension_semantics=("arbitrary",)),
    )(*blocks, *bands)


def per_device(coefficients, vectors):
    rows, cols, _ = vectors.shape
    masked = masked_weights(coefficients)
    halos, near = exchange(vectors, masked)
    ext = jnp.concatenate(
        [
            jnp.concatenate([near[dy, 1], near[dy, 0] if dy else masked, near[dy, -1]], axis=2)
            for dy in (1, 0, -1)
        ],
        axis=1,
    )
    normal, *bands = band_matrices(ext, rows, cols)
    image = image_of(vectors, halos, bands)
    return (normal, image)


def solution(mesh):
    in_specs = (P(None, "gy", "gx"), P("gy", "gx", None))
    out_specs = (P(None, "gy", "gx"), P("gy", "gx", None))
    return jax.shard_map(
        per_device, mesh=mesh, in_specs=in_specs, out_specs=out_specs, check_vma=False
    )
```
